32 devices in a mesh: dp: 8 (over z, core), mp: 4 (over y, x).
Axes of the slice: x: 2, y: 2, z: 4, core: 2. Of those that a mesh axis runs over, the one named last changes fastest.
Arguments:
- hidden_states: bfloat16 [32, 640, 1280], P(('dp', 'mp')), may hold values from -6 to 6
- ln_attn_gain: float32 [1280], replicated, may hold values from 0.1 to 1.9
- w_qkv: bfloat16 [1280, 16, 192], P(None, 'mp'), may hold values from -0.15625 to 0.15625
- output_weight: bfloat16 [64, 16, 1280], P(None, 'mp'), may hold values from -0.75 to 0.75
- ln_final_gain: float32 [1280], replicated, may hold values from 0.1 to 1.9
- dense_weight: bfloat16 [1280, 1280], replicated, may hold values from -0.15625 to 0.15625
- decoder_weight: bfloat16 [1280, 33], replicated, may hold values from -0.5390625 to 0.5390625
- decoder_bias: float32 [33], replicated, may hold values from -4 to 4
- seq_tokens: int32 [24, 640], replicated, may hold values from 4 to 23
- seq_lengths: int32 [24], replicated, may hold values from 128 to 640
- copy_sequence: int32 [32], replicated, may hold values from 0 to 23
- mask_code: int32 [32, 64], replicated, may hold values from 0 to 1048575
- copy_owner: int32 [32], replicated, may hold values from 0 to 31, each once
Outputs:
- pll: float32 [32, 64], P('dp', 'mp')
The draws below stay inside these ranges and needn't reach their ends.
Inputs may be any that keep to these rules, and one draw needn't show every extreme that they name: `seq_tokens`: amino-acid token ids. `copy_owner`: every row of pll is named by exactly one copy.
All inputs are finite; a program needn't handle non-finite values.
Results may differ from the reference program's by a relative error of at most 0.0038.
Values may be sent and summed in bfloat16 or wider, within the bound.
A program may use at most 128 MiB of HBM per device.

```python
import jax
import jax.numpy as jnp
from jax import lax

D = 1280
HD = 64
VOCAB = 33
HEADS = 16
LMAX = 640
MASKS = 64
SEQS = 24
COPIES = 32


def place_ends(entries, own_key, low, high):
    longest = entries.shape.index(max(entries.shape))
    spots = []
    for shift in (0, 1):
        where = [jax.random.randint(jax.random.fold_in(own_key, axis), (), 0, length) for axis, length in enumerate(entries.shape)]
        where[longest] = (where[longest] + shift) % entries.shape[longest]
        spots.append(tuple(where))
    return entries.at[spots[0]].set(low).at[spots[1]].set(high)


def levels(stream_key, dims, split, least, high):
    loudness, own = 1.0, jax.random.fold_in(stream_key, 6)
    for axis_at, blocks in split:
        steps = jnp.exp(jax.random.uniform(jax.random.fold_in(own, axis_at), (blocks,), jnp.float32, least / len(split), high / len(split)))
        loudness = loudness * jnp.repeat(steps, dims[axis_at] // blocks).reshape([-1 if axis == axis_at else 1 for axis in range(len(dims))])
    return loudness


def bell_draw(key, shape, spread, limit, cuts=(), kind=jnp.bfloat16):
    loudness = levels(key, shape, cuts, -0.22, 0.18) if cuts else 1.0
    array = jax.random.normal(key, shape, jnp.float32) * spread * loudness
    return jnp.minimum(jnp.maximum(array, -limit), limit).astype(kind)


def setup_inputs(seed: int = 0) -> dict:
    streams_of = jax.random.split(jax.random.key(seed), 14)
    hidden_states = bell_draw(streams_of[0], (COPIES, LMAX, D), 1.0, 6.0, ((0, 32),))
    ln_attn_gain = jnp.clip(1.0 + 0.18 * jax.random.normal(streams_of[1], (D,), jnp.float32), 0.1, 1.9)
    w_qkv = bell_draw(streams_of[2], (D, HEADS, 3 * HD), D ** -0.5, 0.15625, ((1, 4),))
    output_weight = bell_draw(streams_of[3], (HD, HEADS, D), 0.125, 0.75, ((1, 4),))
    ln_final_gain = jnp.clip(1.0 + 0.18 * jax.random.normal(streams_of[4], (D,), jnp.float32), 0.1, 1.9)
    dense_weight = bell_draw(streams_of[5], (D, D), D ** -0.5, 0.15625)
    decoder_weight = bell_draw(streams_of[6], (D, VOCAB), 0.09, 0.5390625)
    decoder_bias = bell_draw(streams_of[7], (VOCAB,), 1.0, 4.0, (), jnp.float32)
    seq_tokens = place_ends(jax.random.randint(streams_of[8], (SEQS, LMAX), 4, 24), jax.random.fold_in(streams_of[8], 1), 4, 23).astype(jnp.int32)
    seq_lengths = place_ends(jax.random.randint(streams_of[9], (SEQS,), LMAX // 5, LMAX + 1), jax.random.fold_in(streams_of[9], 1), LMAX // 5, LMAX).astype(jnp.int32)
    copy_sequence = place_ends(jax.random.randint(streams_of[10], (COPIES,), 0, SEQS), jax.random.fold_in(streams_of[10], 1), 0, SEQS - 1).astype(jnp.int32)
    mask_code = place_ends(jax.random.randint(streams_of[11], (COPIES, MASKS), 0, 1048576), jax.random.fold_in(streams_of[11], 1), 0, 1048575).astype(jnp.int32)
    copy_owner = jax.random.permutation(streams_of[12], COPIES).astype(jnp.int32)
    return {"hidden_states": hidden_states, "ln_attn_gain": ln_attn_gain, "w_qkv": w_qkv, "output_weight": output_weight, "ln_final_gain": ln_final_gain, "dense_weight": dense_weight, "decoder_weight": decoder_weight, "decoder_bias": decoder_bias, "seq_tokens": seq_tokens, "seq_lengths": seq_lengths, "copy_sequence": copy_sequence, "mask_code": mask_code, "copy_owner": copy_owner}


epsilon = 1e-05

def layer_norm(inputs):
    average = lax.optimization_barrier(jnp.mean(inputs, axis=-1, keepdims=True))
    centred = inputs - average
    variance = lax.optimization_barrier(jnp.mean(centred * centred, axis=-1, keepdims=True))
    return centred * lax.rsqrt(variance + epsilon)

def rotary_tables(seq_span, head_size):
    half_width = head_size // 2
    frequency = 1.0 / 10000.0 ** (jnp.arange(half_width, dtype=jnp.float32) * (2.0 / head_size))
    angles = jnp.arange(seq_span, dtype=jnp.float32)[:, None] * frequency[None, :]
    angles = jnp.concatenate([angles, angles], axis=-1)
    return (jnp.cos(angles), jnp.sin(angles))

def rotate(inputs, cosine, sine):
    half_width = inputs.shape[-1] // 2
    turned = jnp.concatenate([-inputs[..., half_width:], inputs[..., :half_width]], axis=-1)
    return inputs * cosine + turned * sine

def score_rows(residual, ln_final_gain, dense_weight, decoder_weight, decoder_bias, targets):
    feature = residual.shape[-1]
    normed_final = (layer_norm(residual) * ln_final_gain).astype(jnp.bfloat16).reshape(-1, feature)
    dense_out = jnp.dot(normed_final, dense_weight, preferred_element_type=jnp.float32)
    headed = layer_norm(jax.nn.gelu(dense_out, approximate=False)).astype(jnp.bfloat16)
    logits = jnp.dot(headed, decoder_weight, preferred_element_type=jnp.float32) + decoder_bias
    log_probs = logits - jax.nn.logsumexp(logits, axis=-1, keepdims=True)
    vocab_ids = jnp.arange(logits.shape[-1], dtype=jnp.int32)
    flat_targets = targets.reshape(-1)
    picked = lax.optimization_barrier(jnp.sum(jnp.where(flat_targets[:, None] == vocab_ids[None, :], log_probs, 0.0), axis=-1))
    return picked.reshape(targets.shape)

def one_copy(states, length, positions, ln_attn_gain, w_qkv, output_weight, cosine, sine):
    seq_span, feature = states.shape
    head_count = w_qkv.shape[1]
    head_size = w_qkv.shape[2] // 3
    normed = (layer_norm(states.astype(jnp.float32)) * ln_attn_gain).astype(jnp.bfloat16)
    projected = jnp.dot(normed, w_qkv.reshape(feature, -1), preferred_element_type=jnp.float32)
    projected = projected.reshape(seq_span, head_count, 3, head_size)
    key_matrix = rotate(projected[:, :, 1], cosine[:, None, :], sine[:, None, :]).astype(jnp.bfloat16)
    value_matrix = projected[:, :, 2].astype(jnp.bfloat16)
    query_matrix = projected[positions, :, 0] * head_size ** (-0.5)
    query_matrix = rotate(query_matrix, cosine[positions][:, None, :], sine[positions][:, None, :]).astype(jnp.bfloat16)
    attention_logits = jnp.einsum('fop,yop->ofy', query_matrix.astype(jnp.float32), key_matrix.astype(jnp.float32))
    alive = jnp.arange(seq_span, dtype=jnp.int32) < length
    attention_logits = jnp.where(alive[None, None, :], attention_logits, -1e+30)
    largest = lax.optimization_barrier(jnp.max(attention_logits, axis=-1, keepdims=True))
    weights = jnp.exp(attention_logits - largest)
    attention_probs = (weights / lax.optimization_barrier(jnp.sum(weights, axis=-1, keepdims=True))).astype(jnp.bfloat16)
    context_vectors = jnp.einsum('vuy,yvx->uvx', attention_probs.astype(jnp.float32), value_matrix.astype(jnp.float32)).astype(jnp.bfloat16)
    attention_mixed = jnp.einsum('frn,nrl->fl', context_vectors.astype(jnp.float32), output_weight.astype(jnp.float32))
    return states[positions].astype(jnp.float32) + attention_mixed

def reference(hidden_states, ln_attn_gain, w_qkv, output_weight, ln_final_gain, dense_weight, decoder_weight, decoder_bias, seq_tokens, seq_lengths, copy_sequence, mask_code, copy_owner):
    cosine, sine = rotary_tables(LMAX, HD)
    lengths = seq_lengths[copy_sequence]
    positions = (mask_code % lengths[:, None]).astype(jnp.int32)
    targets = jnp.take_along_axis(seq_tokens[copy_sequence], positions, axis=1)

    def per_copy(items):
        states, length, spots = items
        return one_copy(states, length, spots, ln_attn_gain, w_qkv, output_weight, cosine, sine)
    residual = lax.map(per_copy, (hidden_states, lengths, positions))
    attention_logits = score_rows(residual, ln_final_gain, dense_weight, decoder_weight, decoder_bias, targets)
    return jnp.zeros_like(attention_logits).at[copy_owner].set(attention_logits)
```

```python
import functools

import jax
import jax.numpy as jnp
import numpy as np
from jax import lax
from jax.experimental import pallas as pl
from jax.experimental.pallas import tpu as pltpu
from jax.sharding import PartitionSpec as P

epsilon = 1e-05
MESH = pl.DeviceIdType.MESH
f32 = jnp.float32
bf16 = jnp.bfloat16
LANES = 128


def layer_norm(inputs):
    average = jnp.mean(inputs, axis=-1, keepdims=True)
    centred = inputs - average
    variance = jnp.mean(centred * centred, axis=-1, keepdims=True)
    return centred * lax.rsqrt(variance + epsilon)


def rotary_tables(seq_span, head_size):
    half = head_size // 2
    frequency = (1.0 / 10000.0 ** (np.arange(half, dtype=np.float32) * (2.0 / head_size))).astype(
        np.float32
    )
    angles = np.arange(seq_span, dtype=np.float32)[:, None] * frequency[None, :]
    cosine, sine = np.cos(angles), np.sin(angles)
    times = LANES // head_size
    return (
        np.tile(np.concatenate([cosine, cosine], axis=1), (1, times)).astype(np.float32),
        np.tile(np.concatenate([-sine, sine], axis=1), (1, times)).astype(np.float32),
    )


def flip(index, mask):
    bit = 1
    out = index
    while bit <= mask:
        if mask & bit:
            out = out + bit * (1 - 2 * ((index // bit) % 2))
        bit *= 2
    return out


def kernel(
    sizes,
    sequence_ref,
    lengths_ref,
    codes_ref,
    tokens_ref,
    owner_ref,
    gain_ref,
    final_gain_ref,
    decoder_ref,
    bias_ref,
    hidden_hbm,
    weight_hbm,
    out_weight_hbm,
    dense_hbm,
    cos_hbm,
    sin_hbm,
    out_ref,
    hidden,
    normed,
    wbuf,
    obuf,
    dense,
    cos,
    sin,
    pbuf,
    context,
    mixed,
    scores,
    local_sem,
    direct_sem,
    relay_sem,
    share_sem,
    arrive_sem,
    shared_sem,
    score_send_sem,
    score_sem,
):
    n_dp, n_mp, head_size, heads_in_chunk, chunks = sizes
    devices = n_dp * n_mp
    dp = lax.axis_index("dp")
    mp = lax.axis_index("mp")
    core = dp % 2
    partner = dp + 1 - 2 * core
    me = dp * n_mp + mp
    seq_span, feature = hidden.shape
    masks = codes_ref.shape[1]
    chunk_rows = chunk_heads = heads_in_chunk * head_size
    half_rows = feature // 2
    out_rows = obuf.shape[1]
    piece_rows = out_rows // 4

    def local(index, source, target):
        copy = pltpu.make_async_copy(source, target, local_sem.at[index])
        copy.start()
        return copy

    hidden_copy = local(0, hidden_hbm, hidden)
    weight_copy = local(1, weight_hbm, wbuf.at[0])
    out_weight_copy = local(2, out_weight_hbm, obuf.at[0])
    cos_copy = local(3, cos_hbm, cos)
    sin_copy = local(4, sin_hbm, sin)
    dense_copy = local(5, dense_hbm, dense)

    barrier = pltpu.get_barrier_semaphore()

    def greet(step, carry):
        other = (me + step) % devices
        pl.semaphore_signal(
            barrier, inc=1, device_id=(other // n_mp, other % n_mp), device_id_type=MESH
        )
        return carry

    lax.fori_loop(1, devices, greet, 0)

    def view(relation, item):
        if item < chunks:
            return wbuf.at[relation, item, pl.ds(pl.multiple_of(core * half_rows, 16), half_rows), :]
        start = core * (2 * piece_rows) + (item - chunks) * piece_rows
        return obuf.at[relation, pl.ds(pl.multiple_of(start, 16), piece_rows), :]

    def partner_view(relation, item):
        if item < chunks:
            start = (1 - core) * half_rows
            return wbuf.at[relation, item, pl.ds(pl.multiple_of(start, 16), half_rows), :]
        start = (1 - core) * (2 * piece_rows) + (item - chunks) * piece_rows
        return obuf.at[relation, pl.ds(pl.multiple_of(start, 16), piece_rows), :]

    sent = []

    def to_group(target, source_relation, relation, item, semaphore):
        copy = pltpu.make_async_remote_copy(
            src_ref=view(source_relation, item),
            dst_ref=view(relation, item),
            send_sem=semaphore,
            recv_sem=arrive_sem.at[relation, item],
            device_id=(dp, flip(mp, target)),
            device_id_type=MESH,
        )
        copy.start()
        sent.append(copy)

    def direct(target, item):
        to_group(target, 0, target, item, direct_sem.at[target, item])

    def relay(target, source_relation, item):
        to_group(target, source_relation, source_relation ^ target, item, relay_sem.at[item])

    def arrived(relation, item):
        landing = view(relation, item)
        pltpu.make_async_copy(landing, landing, arrive_sem.at[relation, item]).wait()

    def share(relation, item):
        copy = pltpu.make_async_remote_copy(
            src_ref=view(relation, item),
            dst_ref=view(relation, item),
            send_sem=share_sem.at[relation, item],
            recv_sem=shared_sem.at[relation, item],
            device_id=(partner, mp),
            device_id_type=MESH,
        )
        copy.start()
        sent.append(copy)

    def was_shared(relation, item):
        landing = partner_view(relation, item)
        pltpu.make_async_copy(landing, landing, shared_sem.at[relation, item]).wait()

    sequence = sequence_ref[me]
    length = lengths_ref[sequence].astype(f32)
    codes = codes_ref[pl.ds(me, 1), :].astype(f32)
    quotient = jnp.floor(codes / length)
    row_positions = codes - quotient * length
    row_positions = jnp.where(row_positions < 0.0, row_positions + length, row_positions)
    row_positions = jnp.where(row_positions >= length, row_positions - length, row_positions)
    eye = lax.broadcasted_iota(jnp.int32, (masks, masks), 0) == lax.broadcasted_iota(
        jnp.int32, (masks, masks), 1
    )
    positions = jnp.sum(jnp.where(eye, row_positions, 0.0), axis=1, keepdims=True)
    places = lax.broadcasted_iota(jnp.int32, (masks, seq_span), 1).astype(f32)
    chosen = places == positions
    onehot = jnp.where(chosen, 1.0, 0.0)
    onehot_bf = onehot.astype(bf16)
    tokens = tokens_ref[pl.ds(sequence, 1), :].astype(f32)
    targets = jnp.sum(jnp.where(chosen, tokens, 0.0), axis=1, keepdims=True)
    alive = lax.broadcasted_iota(jnp.int32, (1, seq_span), 1).astype(f32) < length

    weight_copy.wait()
    out_weight_copy.wait()
    pl.semaphore_wait(barrier, devices - 1)
    items = chunks + 2
    routed = n_mp == 4 and chunks == 2
    if routed:
        direct(1, 0)
        direct(2, 1)
        direct(1, 1)
        direct(2, 0)
    else:
        for item in range(items):
            for target in range(1, n_mp):
                direct(target, item)

    hidden_copy.wait()
    tile = 128 if seq_span % 128 == 0 else 8

    def norm_rows(step, carry):
        rows = pl.ds(pl.multiple_of(step * tile, tile), tile)
        normed[rows, :] = (layer_norm(hidden[rows, :].astype(f32)) * gain_ref[...]).astype(bf16)
        return carry

    lax.fori_loop(0, seq_span // tile, norm_rows, 0)
    masked_rows = jnp.dot(onehot_bf, normed[...], preferred_element_type=f32).astype(bf16)
    own_rows = jnp.dot(onehot_bf, hidden[...], preferred_element_type=f32)
    mixed[...] = own_rows
    cos_copy.wait()
    sin_copy.wait()
    exact = dict(preferred_element_type=f32, precision=lax.Precision.HIGHEST)
    query_cos = jnp.dot(onehot, cos[...], **exact)
    query_sin = jnp.dot(onehot, sin[...], **exact)
    lane = lax.broadcasted_iota(jnp.int32, (1, LANES), 1)
    first = lane % head_size < head_size // 2

    def rotate(inputs, cosine, sine):
        turned = jnp.where(
            first,
            pltpu.roll(inputs, LANES - head_size // 2, 1),
            pltpu.roll(inputs, head_size // 2, 1),
        )
        return inputs * cosine + turned * sine

    width = wbuf.shape[3]
    span = seq_span // 2 if seq_span % 32 == 0 else seq_span

    def attend(relation, chunk):
        weights = wbuf.at[relation, chunk]

        def project(step, carry):
            rows = pl.ds(pl.multiple_of(step * span, 16), span)
            made = jnp.dot(normed[rows, :], weights[...], preferred_element_type=f32)
            for start in range(0, width, LANES):
                end = min(start + LANES, width)
                part = made[:, start:end]
                keys = [
                    head * 3 * head_size + head_size
                    for head in range(heads_in_chunk)
                    if start <= head * 3 * head_size + head_size < end
                ]
                for key in keys:
                    low = key - start
                    turned = rotate(part, cos[rows, :], sin[rows, :])
                    inside = (lane >= low) & (lane < low + head_size)
                    part = jnp.where(inside, turned, part)
                pbuf[rows, start:end] = part.astype(bf16)
            return carry

        lax.fori_loop(0, seq_span // span, project, 0)
        made = jnp.dot(masked_rows, weights[...], preferred_element_type=f32) * head_size ** (-0.5)
        total = None
        for head in range(heads_in_chunk):
            at = head * 3 * head_size
            block = at // LANES * LANES
            query = rotate(made[:, block : block + LANES], query_cos, query_sin)
            query = pltpu.roll(query, head_size, 1)
            key = at + head_size
            block = key // LANES * LANES
            inside = (lane >= key - block) & (lane < key - block + head_size)
            query = jnp.where(inside, query, 0.0).astype(bf16)
            logits = lax.dot_general(
                query,
                pbuf[:, block : block + LANES],
                (((1,), (1,)), ((), ())),
                preferred_element_type=f32,
            )
            logits = jnp.where(alive, logits, -1e30)
            weight = jnp.exp(logits - jnp.max(logits, axis=-1, keepdims=True))
            probs = (weight / jnp.sum(weight, axis=-1, keepdims=True)).astype(bf16)
            value = at + 2 * head_size
            block = value // LANES * LANES
            end = min(block + LANES, width)
            vectors = jnp.dot(probs, pbuf[:, block:end], preferred_element_type=f32)
            if total is None:
                total = vectors
            else:
                low = value - block
                inside = (lane >= low) & (lane < low + head_size)
                total = jnp.where(inside, vectors, total)
        context[relation, chunk] = total.astype(bf16)

    def mix(relation):
        for chunk in range(chunks):
            rows = slice(chunk * chunk_heads, (chunk + 1) * chunk_heads)
            mixed[...] += jnp.dot(
                context[relation, chunk], obuf[relation, rows, :], preferred_element_type=f32
            )

    def attend_all(pairs):
        for relation, chunk in pairs:
            attend(relation, chunk)

    attend_all([(0, chunk) for chunk in range(chunks)])
    mix(0)

    def fetch(pairs, relays=()):
        for pair in pairs:
            arrived(*pair)
            for target, source_relation, item in relays:
                if (source_relation, item) == pair:
                    relay(target, source_relation, item)
            share(*pair)

    if routed:
        relays = [(1, 2, 1), (2, 1, 0), (1, 2, chunks + 1), (2, 1, chunks)]
        fetch([(1, 0), (2, 1)], relays)
        for item in (chunks, chunks + 1):
            direct(1, 2 * chunks + 1 - item)
            direct(2, item)
        for pair in [(1, 0), (2, 1)]:
            was_shared(*pair)
            attend(*pair)
        fetch([(1, 1), (2, 0)], relays)
        for pair in [(1, 1), (2, 0)]:
            was_shared(*pair)
            attend(*pair)
        fetch([(3, 0), (3, 1)])
        for pair in [(3, 0), (3, 1)]:
            was_shared(*pair)
            attend(*pair)
        fetch([(1, chunks), (2, chunks + 1), (1, chunks + 1), (2, chunks)], relays)
        fetch([(3, chunks), (3, chunks + 1)])
        for relation in (1, 2, 3):
            was_shared(relation, chunks)
            was_shared(relation, chunks + 1)
            mix(relation)
    else:
        for relation in range(1, n_mp):
            fetch([(relation, item) for item in range(items)])
        for relation in range(1, n_mp):
            for item in range(items):
                was_shared(relation, item)
            attend_all([(relation, chunk) for chunk in range(chunks)])
            mix(relation)

    normed_final = (layer_norm(mixed[...]) * final_gain_ref[...]).astype(bf16)
    dense_copy.wait()
    dense_out = jnp.dot(normed_final, dense[...], preferred_element_type=f32)
    headed = layer_norm(0.5 * dense_out * (1.0 + lax.erf(dense_out * 0.5**0.5))).astype(bf16)
    logits = jnp.dot(headed, decoder_ref[...], preferred_element_type=f32) + bias_ref[...]
    largest = jnp.max(logits, axis=-1, keepdims=True)
    scale = jnp.log(jnp.sum(jnp.exp(logits - largest), axis=-1, keepdims=True)) + largest
    vocabulary = lax.broadcasted_iota(jnp.int32, logits.shape, 1).astype(f32)
    picked = jnp.sum(jnp.where(vocabulary == targets, logits - scale, 0.0), axis=1, keepdims=True)
    row = jnp.sum(jnp.where(eye, picked, 0.0), axis=0, keepdims=True)
    padded = jnp.concatenate([row, jnp.zeros((1, LANES - masks), f32)], axis=1) if masks < LANES else row
    scores[me] = jnp.broadcast_to(padded, scores.shape[1:])

    def score_copy(step):
        other = (me + step) % devices
        return pltpu.make_async_remote_copy(
            src_ref=scores.at[me],
            dst_ref=scores.at[me],
            send_sem=score_send_sem.at[step],
            recv_sem=score_sem.at[me],
            device_id=(other // n_mp, other % n_mp),
            device_id_type=MESH,
        )

    def send_scores(step, carry):
        score_copy(step).start()
        return carry

    lax.fori_loop(1, devices, send_scores, 0)
    for copy in sent:
        copy.wait_send()

    def wait_scores(step, carry):
        source = (me + step) % devices
        landing = scores.at[source]
        pltpu.make_async_copy(landing, landing, score_sem.at[source]).wait()
        return carry

    lax.fori_loop(1, devices, wait_scores, 0)

    def wait_sends(step, carry):
        score_copy(step).wait_send()
        return carry

    lax.fori_loop(1, devices, wait_sends, 0)
    group = out_ref.shape[0]
    wanted = dp * group + lax.broadcasted_iota(jnp.int32, (group, owner_ref.shape[1]), 0)
    select = jnp.where(owner_ref[...] == wanted, 1.0, 0.0)
    out_ref[...] = jnp.dot(select, scores[:, 0, :], **exact)


def on_device(
    shape,
    hidden_states,
    ln_attn_gain,
    w_qkv,
    output_weight,
    ln_final_gain,
    dense_weight,
    decoder_weight,
    decoder_bias,
    seq_tokens,
    seq_lengths,
    copy_sequence,
    mask_code,
    copy_owner,
):
    n_dp, n_mp = shape
    devices = n_dp * n_mp
    lane_copies, seq_span, feature = hidden_states.shape
    head_size, heads, _ = output_weight.shape
    copies, masks = mask_code.shape
    assert lane_copies == 1 and copies == devices and n_dp % 2 == 0
    in_chunk = 2 if heads % 2 == 0 else 1
    chunks = heads // in_chunk
    width = in_chunk * 3 * head_size
    weight = jnp.swapaxes(w_qkv.reshape(feature, chunks, width), 0, 1)
    out_weight = jnp.swapaxes(output_weight, 0, 1).reshape(heads * head_size, feature)
    cosine, sine = rotary_tables(seq_span, head_size)
    group = copies // n_dp
    items = chunks + 2
    dma = pltpu.SemaphoreType.DMA
    vmem = pl.BlockSpec(memory_space=pltpu.VMEM)
    smem = pl.BlockSpec(memory_space=pltpu.SMEM)
    anywhere = pl.BlockSpec(memory_space=pl.ANY)
    rows = pl.pallas_call(
        functools.partial(kernel, (n_dp, n_mp, head_size, in_chunk, chunks)),
        name="score_copies",
        out_shape=jax.ShapeDtypeStruct((group, LANES), f32),
        in_specs=[smem] * 2 + [vmem] * 7 + [anywhere] * 6,
        out_specs=vmem,
        scratch_shapes=[
            pltpu.VMEM((seq_span, feature), bf16),
            pltpu.VMEM((seq_span, feature), bf16),
            pltpu.VMEM((n_mp, chunks, feature, width), bf16),
            pltpu.VMEM((n_mp, heads * head_size, feature), bf16),
            pltpu.VMEM((feature, feature), bf16),
            pltpu.VMEM((seq_span, LANES), f32),
            pltpu.VMEM((seq_span, LANES), f32),
            pltpu.VMEM((seq_span, width), bf16),
            pltpu.VMEM((n_mp, chunks, masks, in_chunk * head_size), bf16),
            pltpu.VMEM((masks, feature), f32),
            pltpu.VMEM((devices, 8, LANES), f32),
            dma((6,)),
            dma((n_mp, items)),
            dma((items,)),
            dma((n_mp, items)),
            dma((n_mp, items)),
            dma((n_mp, items)),
            dma((devices,)),
            dma((devices,)),
        ],
        compiler_params=pltpu.CompilerParams(collective_id=0, has_side_effects=True),
    )(
        copy_sequence,
        seq_lengths,
        mask_code,
        seq_tokens,
        copy_owner.reshape(1, -1),
        ln_attn_gain.reshape(1, -1),
        ln_final_gain.reshape(1, -1),
        decoder_weight,
        decoder_bias.reshape(1, -1),
        hidden_states.reshape(seq_span, feature),
        weight,
        out_weight,
        dense_weight,
        jnp.asarray(cosine),
        jnp.asarray(sine),
    )
    own = masks // n_mp
    return lax.dynamic_slice_in_dim(rows, lax.axis_index("mp") * own, own, 1)


def solution(mesh):
    placed = (
        P(("dp", "mp"), None, None),
        P(),
        P(None, "mp", None),
        P(None, "mp", None),
        P(),
        P(),
        P(),
        P(),
        P(),
        P(),
        P(),
        P(),
        P(),
    )
    shape = (mesh.shape["dp"], mesh.shape["mp"])
    return jax.shard_map(
        functools.partial(on_device, shape),
        mesh=mesh,
        in_specs=placed,
        out_specs=P("dp", "mp"),
        check_vma=False,
    )
```

```python
import functools

import jax
import jax.numpy as jnp
import numpy as np
from jax import lax
from jax.experimental import pallas as pl
from jax.experimental.pallas import tpu as pltpu
from jax.sharding import PartitionSpec as P

epsilon = 1e-05
MESH = pl.DeviceIdType.MESH
f32 = jnp.float32
bf16 = jnp.bfloat16
LANES = 128


def layer_norm(inputs):
    average = jnp.mean(inputs, axis=-1, keepdims=True)
    centred = inputs - average
    variance = jnp.mean(centred * centred, axis=-1, keepdims=True)
    return centred * lax.rsqrt(variance + epsilon)


def rotary_tables(seq_span, head_size):
    half = head_size // 2
    frequency = (1.0 / 10000.0 ** (np.arange(half, dtype=np.float32) * (2.0 / head_size))).astype(
        np.float32
    )
    angles = np.arange(seq_span, dtype=np.float32)[:, None] * frequency[None, :]
    cosine, sine = np.cos(angles), np.sin(angles)
    times = LANES // head_size
    return (
        np.tile(np.concatenate([cosine, cosine], axis=1), (1, times)).astype(np.float32),
        np.tile(np.concatenate([-sine, sine], axis=1), (1, times)).astype(np.float32),
    )


def flip(index, mask):
    bit = 1
    out = index
    while bit <= mask:
        if mask & bit:
            out = out + bit * (1 - 2 * ((index // bit) % 2))
        bit *= 2
    return out


def kernel(
    sizes,
    sequence_ref,
    lengths_ref,
    codes_ref,
    tokens_ref,
    owner_ref,
    gain_ref,
    final_gain_ref,
    decoder_ref,
    bias_ref,
    hidden_hbm,
    weight_hbm,
    out_weight_hbm,
    dense_hbm,
    cos_hbm,
    sin_hbm,
    out_ref,
    hidden,
    normed,
    wbuf,
    obuf,
    dense,
    cos,
    sin,
    pbuf,
    context,
    mixed,
    scores,
    local_sem,
    direct_sem,
    relay_sem,
    exchange_sem,
    share_sem,
    arrive_sem,
    shared_sem,
    score_send_sem,
    score_sem,
):
    n_dp, n_mp, head_size, heads_in_chunk, chunks = sizes
    devices = n_dp * n_mp
    dp = lax.axis_index("dp")
    mp = lax.axis_index("mp")
    core = dp % 2
    partner = dp + 1 - 2 * core
    me = dp * n_mp + mp
    seq_span, feature = hidden.shape
    masks = codes_ref.shape[1]
    chunk_heads = heads_in_chunk * head_size
    out_rows = obuf.shape[1]
    piece_rows = out_rows // 4

    def local(index, source, target):
        copy = pltpu.make_async_copy(source, target, local_sem.at[index])
        copy.start()
        return copy

    hidden_copy = local(0, hidden_hbm, hidden)
    weight_copy = local(1, weight_hbm, wbuf.at[0])
    out_weight_copy = local(2, out_weight_hbm, obuf.at[0])
    cos_copy = local(3, cos_hbm, cos)
    sin_copy = local(4, sin_hbm, sin)
    dense_copy = local(5, dense_hbm, dense)

    barrier = pltpu.get_barrier_semaphore()

    def greet(step, carry):
        other = (me + step) % devices
        pl.semaphore_signal(
            barrier, inc=1, device_id=(other // n_mp, other % n_mp), device_id_type=MESH
        )
        return carry

    lax.fori_loop(1, devices, greet, 0)

    parity = (dp // 2) % 2
    above = dp + 2 - 4 * parity
    part_rows = wbuf.shape[2] // 4

    def part(chunk, odd):
        return 2 * chunk + odd

    def place(relation, item, half):
        if item < 2 * chunks:
            chunk, odd = divmod(item, 2)
            which = 1 - parity if odd else parity
            start = (2 * half + which) * part_rows
            return wbuf.at[relation, chunk, pl.ds(pl.multiple_of(start, 16), part_rows), :]
        start = (2 * half + item - 2 * chunks) * piece_rows
        return obuf.at[relation, pl.ds(pl.multiple_of(start, 16), piece_rows), :]

    def view(relation, item):
        return place(relation, item, core)

    def partner_view(relation, item):
        return place(relation, item, 1 - core)

    sent = []

    def to_group(target, source_relation, relation, item, semaphore):
        copy = pltpu.make_async_remote_copy(
            src_ref=view(source_relation, item),
            dst_ref=view(relation, item),
            send_sem=semaphore,
            recv_sem=arrive_sem.at[relation, item],
            device_id=(dp, flip(mp, target)),
            device_id_type=MESH,
        )
        copy.start()
        sent.append(copy)

    def direct(target, item):
        to_group(target, 0, target, item, direct_sem.at[target, item])

    def relay(target, source_relation, item):
        to_group(target, source_relation, source_relation ^ target, item, relay_sem.at[item])

    def exchange(relation, chunk):
        copy = pltpu.make_async_remote_copy(
            src_ref=view(relation, part(chunk, 0)),
            dst_ref=view(relation, part(chunk, 0)),
            send_sem=exchange_sem.at[relation, chunk],
            recv_sem=arrive_sem.at[relation, part(chunk, 1)],
            device_id=(above, mp),
            device_id_type=MESH,
        )
        copy.start()
        sent.append(copy)

    def arrived(relation, item):
        landing = view(relation, item)
        pltpu.make_async_copy(landing, landing, arrive_sem.at[relation, item]).wait()

    def share(relation, item):
        copy = pltpu.make_async_remote_copy(
            src_ref=view(relation, item),
            dst_ref=view(relation, item),
            send_sem=share_sem.at[relation, item],
            recv_sem=shared_sem.at[relation, item],
            device_id=(partner, mp),
            device_id_type=MESH,
        )
        copy.start()
        sent.append(copy)

    def was_shared(relation, item):
        landing = partner_view(relation, item)
        pltpu.make_async_copy(landing, landing, shared_sem.at[relation, item]).wait()

    sequence = sequence_ref[me]
    length = lengths_ref[sequence].astype(f32)
    codes = codes_ref[pl.ds(me, 1), :].astype(f32)
    quotient = jnp.floor(codes / length)
    row_positions = codes - quotient * length
    row_positions = jnp.where(row_positions < 0.0, row_positions + length, row_positions)
    row_positions = jnp.where(row_positions >= length, row_positions - length, row_positions)
    eye = lax.broadcasted_iota(jnp.int32, (masks, masks), 0) == lax.broadcasted_iota(
        jnp.int32, (masks, masks), 1
    )
    positions = jnp.sum(jnp.where(eye, row_positions, 0.0), axis=1, keepdims=True)
    places = lax.broadcasted_iota(jnp.int32, (masks, seq_span), 1).astype(f32)
    chosen = places == positions
    onehot = jnp.where(chosen, 1.0, 0.0)
    onehot_bf = onehot.astype(bf16)
    tokens = tokens_ref[pl.ds(sequence, 1), :].astype(f32)
    targets = jnp.sum(jnp.where(chosen, tokens, 0.0), axis=1, keepdims=True)
    alive = lax.broadcasted_iota(jnp.int32, (1, seq_span), 1).astype(f32) < length

    weight_copy.wait()
    out_weight_copy.wait()
    pl.semaphore_wait(barrier, devices - 1)
    items = 2 * chunks + 2
    routed = n_mp == 4 and chunks == 2 and n_dp % 4 == 0
    if routed:
        direct(1, part(1, 0))
        direct(2, part(0, 0))
        direct(1, part(0, 0))
        direct(2, part(1, 0))
    else:
        for item in range(items):
            for target in range(1, n_mp):
                direct(target, item)

    hidden_copy.wait()
    tile = 128 if seq_span % 128 == 0 else 8

    def norm_rows(step, carry):
        rows = pl.ds(pl.multiple_of(step * tile, tile), tile)
        normed[rows, :] = (layer_norm(hidden[rows, :].astype(f32)) * gain_ref[...].reshape(1, feature)).astype(bf16)
        return carry

    lax.fori_loop(0, seq_span // tile, norm_rows, 0)
    masked_rows = jnp.dot(onehot_bf, normed[...], preferred_element_type=f32).astype(bf16)
    own_rows = jnp.dot(onehot_bf, hidden[...], preferred_element_type=f32)
    mixed[...] = own_rows
    cos_copy.wait()
    sin_copy.wait()
    exact = dict(preferred_element_type=f32, precision=lax.Precision.HIGHEST)
    query_cos = jnp.dot(onehot, cos[...], **exact)
    query_sin = jnp.dot(onehot, sin[...], **exact)
    lane = lax.broadcasted_iota(jnp.int32, (1, LANES), 1)
    first = lane % head_size < head_size // 2

    def rotate(inputs, cosine, sine):
        turned = jnp.where(
            first,
            pltpu.roll(inputs, LANES - head_size // 2, 1),
            pltpu.roll(inputs, head_size // 2, 1),
        )
        return inputs * cosine + turned * sine

    width = wbuf.shape[2]
    transposed = (((1,), (1,)), ((), ()))
    span = seq_span // 2 if seq_span % 32 == 0 else seq_span

    def attend(relation, chunk):
        weights = wbuf.at[relation, chunk]

        def project(step, carry):
            rows = pl.ds(pl.multiple_of(step * span, 16), span)
            made = lax.dot_general(normed[rows, :], weights[...], transposed, preferred_element_type=f32)
            for start in range(0, width, LANES):
                end = min(start + LANES, width)
                part = made[:, start:end]
                keys = [
                    head * 3 * head_size + head_size
                    for head in range(heads_in_chunk)
                    if start <= head * 3 * head_size + head_size < end
                ]
                for key in keys:
                    low = key - start
                    turned = rotate(part, cos[rows, :], sin[rows, :])
                    inside = (lane >= low) & (lane < low + head_size)
                    part = jnp.where(inside, turned, part)
                pbuf[rows, start:end] = part.astype(bf16)
            return carry

        lax.fori_loop(0, seq_span // span, project, 0)
        made = lax.dot_general(masked_rows, weights[...], transposed, preferred_element_type=f32)
        made = made * head_size ** (-0.5)
        total = None
        for head in range(heads_in_chunk):
            at = head * 3 * head_size
            block = at // LANES * LANES
            query = rotate(made[:, block : block + LANES], query_cos, query_sin)
            query = pltpu.roll(query, head_size, 1)
            key = at + head_size
            block = key // LANES * LANES
            inside = (lane >= key - block) & (lane < key - block + head_size)
            query = jnp.where(inside, query, 0.0).astype(bf16)
            logits = lax.dot_general(
                query,
                pbuf[:, block : block + LANES],
                transposed,
                preferred_element_type=f32,
            )
            logits = jnp.where(alive, logits, -1e30)
            weight = jnp.exp(logits - jnp.max(logits, axis=-1, keepdims=True))
            probs = (weight / jnp.sum(weight, axis=-1, keepdims=True)).astype(bf16)
            value = at + 2 * head_size
            block = value // LANES * LANES
            end = min(block + LANES, width)
            vectors = jnp.dot(probs, pbuf[:, block:end], preferred_element_type=f32)
            if total is None:
                total = vectors
            else:
                low = value - block
                inside = (lane >= low) & (lane < low + head_size)
                total = jnp.where(inside, vectors, total)
        context[relation, chunk] = total.astype(bf16)

    def mix(relation):
        for chunk in range(chunks):
            rows = slice(chunk * chunk_heads, (chunk + 1) * chunk_heads)
            mixed[...] += jnp.dot(
                context[relation, chunk], obuf[relation, rows, :], preferred_element_type=f32
            )

    def fetch(*pairs):
        for pair in pairs:
            arrived(*pair)
            share(*pair)

    def attend_shared(relation, chunk):
        was_shared(relation, part(chunk, 0))
        was_shared(relation, part(chunk, 1))
        attend(relation, chunk)

    attend(0, 0)
    if routed:
        first_piece, second_piece = 2 * chunks, 2 * chunks + 1
        arrived(1, part(1, 0))
        relay(2, 1, part(1, 0))
        exchange(1, 1)
        share(1, part(1, 0))
        arrived(2, part(0, 0))
        relay(1, 2, part(0, 0))
        exchange(2, 0)
        share(2, part(0, 0))
        direct(1, part(0, 1))
        direct(2, part(1, 1))
        direct(1, first_piece)
        direct(2, second_piece)
        direct(1, second_piece)
        direct(2, first_piece)
    for chunk in range(1, chunks):
        attend(0, chunk)
    mix(0)
    if routed:
        fetch((1, part(0, 0)), (2, part(1, 0)), (1, part(1, 1)))
        arrived(3, part(0, 0))
        exchange(3, 0)
        share(3, part(0, 0))
        arrived(3, part(1, 0))
        exchange(3, 1)
        share(3, part(1, 0))
        fetch((2, part(0, 1)))
        attend_shared(1, 1)
        attend_shared(2, 0)
        fetch((1, part(0, 1)), (2, part(1, 1)), (3, part(0, 1)))
        attend_shared(1, 0)
        arrived(1, first_piece)
        relay(2, 1, first_piece)
        share(1, first_piece)
        arrived(2, second_piece)
        relay(1, 2, second_piece)
        share(2, second_piece)
        attend_shared(2, 1)
        fetch((3, part(1, 1)))
        attend_shared(3, 0)
        fetch((1, second_piece), (2, first_piece))
        attend_shared(3, 1)
        for relation in (1, 2):
            was_shared(relation, first_piece)
            was_shared(relation, second_piece)
            mix(relation)
        fetch((3, first_piece), (3, second_piece))
        was_shared(3, first_piece)
        was_shared(3, second_piece)
        mix(3)
    else:
        for relation in range(1, n_mp):
            fetch(*[(relation, item) for item in range(items)])
        for relation in range(1, n_mp):
            for item in range(items):
                was_shared(relation, item)
            for chunk in range(chunks):
                attend(relation, chunk)
            mix(relation)

    normed_final = (layer_norm(mixed[...]) * final_gain_ref[...].reshape(1, feature)).astype(bf16)
    dense_copy.wait()
    dense_out = jnp.dot(normed_final, dense[...], preferred_element_type=f32)
    headed = layer_norm(0.5 * dense_out * (1.0 + lax.erf(dense_out * 0.5**0.5))).astype(bf16)
    logits = lax.dot_general(headed, decoder_ref[...], transposed, preferred_element_type=f32) + bias_ref[...]
    largest = jnp.max(logits, axis=-1, keepdims=True)
    scale = jnp.log(jnp.sum(jnp.exp(logits - largest), axis=-1, keepdims=True)) + largest
    vocabulary = lax.broadcasted_iota(jnp.int32, logits.shape, 1).astype(f32)
    picked = jnp.sum(jnp.where(vocabulary == targets, logits - scale, 0.0), axis=1, keepdims=True)
    row = jnp.sum(jnp.where(eye, picked, 0.0), axis=0, keepdims=True)
    padded = jnp.concatenate([row, jnp.zeros((1, LANES - masks), f32)], axis=1) if masks < LANES else row
    scores[me] = jnp.broadcast_to(padded, scores.shape[1:])

    def score_copy(step):
        other = (me + step) % devices
        return pltpu.make_async_remote_copy(
            src_ref=scores.at[me],
            dst_ref=scores.at[me],
            send_sem=score_send_sem.at[step],
            recv_sem=score_sem.at[me],
            device_id=(other // n_mp, other % n_mp),
            device_id_type=MESH,
        )

    def send_scores(step, carry):
        score_copy(step).start()
        return carry

    lax.fori_loop(1, devices, send_scores, 0)
    for copy in sent:
        copy.wait_send()

    def wait_scores(step, carry):
        source = (me + step) % devices
        landing = scores.at[source]
        pltpu.make_async_copy(landing, landing, score_sem.at[source]).wait()
        return carry

    lax.fori_loop(1, devices, wait_scores, 0)

    def wait_sends(step, carry):
        score_copy(step).wait_send()
        return carry

    lax.fori_loop(1, devices, wait_sends, 0)
    group = out_ref.shape[0]
    wanted = dp * group + lax.broadcasted_iota(jnp.int32, (group, owner_ref.shape[1]), 0)
    select = jnp.where(owner_ref[...] == wanted, 1.0, 0.0)
    out_ref[...] = jnp.dot(select, scores[:, 0, :], **exact)


def on_device(
    shape,
    hidden_states,
    ln_attn_gain,
    w_qkv,
    output_weight,
    ln_final_gain,
    dense_weight,
    decoder_weight,
    decoder_bias,
    seq_tokens,
    seq_lengths,
    copy_sequence,
    mask_code,
    copy_owner,
):
    n_dp, n_mp = shape
    devices = n_dp * n_mp
    lane_copies, seq_span, feature = hidden_states.shape
    head_size, heads, _ = output_weight.shape
    copies, masks = mask_code.shape
    assert lane_copies == 1 and copies == devices and n_dp % 2 == 0
    in_chunk = 2 if heads % 2 == 0 else 1
    chunks = heads // in_chunk
    width = in_chunk * 3 * head_size
    weight = jnp.transpose(w_qkv.reshape(feature, chunks, width), (1, 2, 0))
    out_weight = jnp.swapaxes(output_weight, 0, 1).reshape(heads * head_size, feature)
    cosine, sine = rotary_tables(seq_span, head_size)
    group = copies // n_dp
    items = 2 * chunks + 2
    dma = pltpu.SemaphoreType.DMA
    vmem = pl.BlockSpec(memory_space=pltpu.VMEM)
    smem = pl.BlockSpec(memory_space=pltpu.SMEM)
    anywhere = pl.BlockSpec(memory_space=pl.ANY)
    rows = pl.pallas_call(
        functools.partial(kernel, (n_dp, n_mp, head_size, in_chunk, chunks)),
        name="score_copies",
        out_shape=jax.ShapeDtypeStruct((group, LANES), f32),
        in_specs=[smem] * 2 + [vmem] * 7 + [anywhere] * 6,
        out_specs=vmem,
        scratch_shapes=[
            pltpu.VMEM((seq_span, feature), bf16),
            pltpu.VMEM((seq_span, feature), bf16),
            pltpu.VMEM((n_mp, chunks, width, feature), bf16),
            pltpu.VMEM((n_mp, heads * head_size, feature), bf16),
            pltpu.VMEM((feature, feature), bf16),
            pltpu.VMEM((seq_span, LANES), f32),
            pltpu.VMEM((seq_span, LANES), f32),
            pltpu.VMEM((seq_span, width), bf16),
            pltpu.VMEM((n_mp, chunks, masks, in_chunk * head_size), bf16),
            pltpu.VMEM((masks, feature), f32),
            pltpu.VMEM((devices, 8, LANES), f32),
            dma((6,)),
            dma((n_mp, items)),
            dma((items,)),
            dma((n_mp, chunks)),
            dma((n_mp, items)),
            dma((n_mp, items)),
            dma((n_mp, items)),
            dma((devices,)),
            dma((devices,)),
        ],
        compiler_params=pltpu.CompilerParams(collective_id=0, has_side_effects=True),
    )(
        copy_sequence,
        seq_lengths,
        mask_code,
        seq_tokens,
        copy_owner.reshape(1, -1),
        ln_attn_gain,
        ln_final_gain,
        decoder_weight.T,
        decoder_bias.reshape(1, -1),
        hidden_states.reshape(seq_span, feature),
        weight,
        out_weight,
        dense_weight,
        jnp.asarray(cosine),
        jnp.asarray(sine),
    )
    own = masks // n_mp
    return lax.dynamic_slice_in_dim(rows, lax.axis_index("mp") * own, own, 1)


def solution(mesh):
    placed = (
        P(("dp", "mp"), None, None),
        P(),
        P(None, "mp", None),
        P(None, "mp", None),
        P(),
        P(),
        P(),
        P(),
        P(),
        P(),
        P(),
        P(),
        P(),
    )
    shape = (mesh.shape["dp"], mesh.shape["mp"])
    return jax.shard_map(
        functools.partial(on_device, shape),
        mesh=mesh,
        in_specs=placed,
        out_specs=P("dp", "mp"),
        check_vma=False,
    )
```

```python
import functools

import jax
import jax.numpy as jnp
import numpy as np
from jax import lax
from jax.experimental import pallas as pl
from jax.experimental.pallas import tpu as pltpu
from jax.sharding import PartitionSpec as P

epsilon = 1e-05
MESH = pl.DeviceIdType.MESH
f32 = jnp.float32
bf16 = jnp.bfloat16
LANES = 128


def layer_norm(inputs):
    average = jnp.mean(inputs, axis=-1, keepdims=True)
    centred = inputs - average
    variance = jnp.mean(centred * centred, axis=-1, keepdims=True)
    return centred * lax.rsqrt(variance + epsilon)


def rotary_tables(seq_span, head_size):
    half = head_size // 2
    frequency = (1.0 / 10000.0 ** (np.arange(half, dtype=np.float32) * (2.0 / head_size))).astype(
        np.float32
    )
    angles = np.arange(seq_span, dtype=np.float32)[:, None] * frequency[None, :]
    cosine, sine = np.cos(angles), np.sin(angles)
    times = LANES // head_size
    return (
        np.tile(np.concatenate([cosine, cosine], axis=1), (1, times)).astype(np.float32),
        np.tile(np.concatenate([-sine, sine], axis=1), (1, times)).astype(np.float32),
    )


def flip(index, mask):
    bit = 1
    out = index
    while bit <= mask:
        if mask & bit:
            out = out + bit * (1 - 2 * ((index // bit) % 2))
        bit *= 2
    return out


def kernel(
    sizes,
    sequence_ref,
    lengths_ref,
    codes_ref,
    tokens_ref,
    owner_ref,
    gain_ref,
    final_gain_ref,
    decoder_ref,
    bias_ref,
    hidden_hbm,
    weight_hbm,
    out_weight_hbm,
    dense_hbm,
    cos_hbm,
    sin_hbm,
    out_ref,
    hidden,
    normed,
    wbuf,
    obuf,
    dense,
    cos,
    sin,
    pbuf,
    context,
    mixed,
    scores,
    local_sem,
    direct_sem,
    relay_sem,
    exchange_sem,
    share_sem,
    arrive_sem,
    shared_sem,
    score_send_sem,
    score_sem,
):
    n_dp, n_mp, head_size, heads_in_chunk, chunks = sizes
    devices = n_dp * n_mp
    dp = lax.axis_index("dp")
    mp = lax.axis_index("mp")
    core = dp % 2
    partner = dp + 1 - 2 * core
    me = dp * n_mp + mp
    seq_span, feature = hidden.shape
    masks = codes_ref.shape[1]
    chunk_heads = heads_in_chunk * head_size
    out_rows = obuf.shape[1]
    piece_rows = out_rows // 4

    def local(index, source, target):
        copy = pltpu.make_async_copy(source, target, local_sem.at[index])
        copy.start()
        return copy

    hidden_copy = local(0, hidden_hbm, hidden)
    weight_copy = local(1, weight_hbm, wbuf.at[0])
    out_weight_copy = local(2, out_weight_hbm, obuf.at[0])
    cos_copy = local(3, cos_hbm, cos)
    sin_copy = local(4, sin_hbm, sin)
    dense_copy = local(5, dense_hbm, dense)

    barrier = pltpu.get_barrier_semaphore()

    def greet(step, carry):
        other = (me + step) % devices
        pl.semaphore_signal(
            barrier, inc=1, device_id=(other // n_mp, other % n_mp), device_id_type=MESH
        )
        return carry

    lax.fori_loop(1, devices, greet, 0)

    parity = (dp // 2) % 2
    above = dp + 2 - 4 * parity
    part_rows = wbuf.shape[2] // 4

    def part(chunk, odd):
        return 2 * chunk + odd

    def place(relation, item, half):
        if item < 2 * chunks:
            chunk, odd = divmod(item, 2)
            which = 1 - parity if odd else parity
            start = (2 * half + which) * part_rows
            return wbuf.at[relation, chunk, pl.ds(pl.multiple_of(start, 16), part_rows), :]
        start = (2 * half + item - 2 * chunks) * piece_rows
        return obuf.at[relation, pl.ds(pl.multiple_of(start, 16), piece_rows), :]

    def view(relation, item):
        return place(relation, item, core)

    def partner_view(relation, item):
        return place(relation, item, 1 - core)

    sent = []

    def to_group(target, source_relation, relation, item, semaphore):
        copy = pltpu.make_async_remote_copy(
            src_ref=view(source_relation, item),
            dst_ref=view(relation, item),
            send_sem=semaphore,
            recv_sem=arrive_sem.at[relation, item],
            device_id=(dp, flip(mp, target)),
            device_id_type=MESH,
        )
        copy.start()
        sent.append(copy)

    def direct(target, item):
        to_group(target, 0, target, item, direct_sem.at[target, item])

    def relay(target, source_relation, item):
        to_group(target, source_relation, source_relation ^ target, item, relay_sem.at[item])

    def exchange(relation, chunk):
        copy = pltpu.make_async_remote_copy(
            src_ref=view(relation, part(chunk, 0)),
            dst_ref=view(relation, part(chunk, 0)),
            send_sem=exchange_sem.at[relation, chunk],
            recv_sem=arrive_sem.at[relation, part(chunk, 1)],
            device_id=(above, mp),
            device_id_type=MESH,
        )
        copy.start()
        sent.append(copy)

    def arrived(relation, item):
        landing = view(relation, item)
        pltpu.make_async_copy(landing, landing, arrive_sem.at[relation, item]).wait()

    def share(relation, item):
        copy = pltpu.make_async_remote_copy(
            src_ref=view(relation, item),
            dst_ref=view(relation, item),
            send_sem=share_sem.at[relation, item],
            recv_sem=shared_sem.at[relation, item],
            device_id=(partner, mp),
            device_id_type=MESH,
        )
        copy.start()
        sent.append(copy)

    def was_shared(relation, item):
        landing = partner_view(relation, item)
        pltpu.make_async_copy(landing, landing, shared_sem.at[relation, item]).wait()

    sequence = sequence_ref[me]
    length = lengths_ref[sequence].astype(f32)
    codes = codes_ref[pl.ds(me, 1), :].astype(f32)
    quotient = jnp.floor(codes / length)
    row_positions = codes - quotient * length
    row_positions = jnp.where(row_positions < 0.0, row_positions + length, row_positions)
    row_positions = jnp.where(row_positions >= length, row_positions - length, row_positions)
    eye = lax.broadcasted_iota(jnp.int32, (masks, masks), 0) == lax.broadcasted_iota(
        jnp.int32, (masks, masks), 1
    )
    positions = jnp.sum(jnp.where(eye, row_positions, 0.0), axis=1, keepdims=True)
    places = lax.broadcasted_iota(jnp.int32, (masks, seq_span), 1).astype(f32)
    chosen = places == positions
    onehot = jnp.where(chosen, 1.0, 0.0)
    onehot_bf = onehot.astype(bf16)
    tokens = tokens_ref[pl.ds(sequence, 1), :].astype(f32)
    targets = jnp.sum(jnp.where(chosen, tokens, 0.0), axis=1, keepdims=True)
    alive = lax.broadcasted_iota(jnp.int32, (1, seq_span), 1).astype(f32) < length

    weight_copy.wait()
    out_weight_copy.wait()
    pl.semaphore_wait(barrier, devices - 1)
    items = 2 * chunks + 2
    routed = n_mp == 4 and chunks == 2 and n_dp % 4 == 0
    if routed:
        direct(1, part(1, 0))
        direct(2, part(0, 0))
        direct(1, part(0, 0))
        direct(2, part(1, 0))
    else:
        for item in range(items):
            for target in range(1, n_mp):
                direct(target, item)

    hidden_copy.wait()
    tile = 128 if seq_span % 128 == 0 else 8

    def norm_rows(step, carry):
        rows = pl.ds(pl.multiple_of(step * tile, tile), tile)
        normed[rows, :] = (layer_norm(hidden[rows, :].astype(f32)) * gain_ref[...].reshape(1, feature)).astype(bf16)
        return carry

    lax.fori_loop(0, seq_span // tile, norm_rows, 0)
    masked_rows = jnp.dot(onehot_bf, normed[...], preferred_element_type=f32).astype(bf16)
    own_rows = jnp.dot(onehot_bf, hidden[...], preferred_element_type=f32)
    mixed[...] = own_rows
    cos_copy.wait()
    sin_copy.wait()
    exact = dict(preferred_element_type=f32, precision=lax.Precision.HIGHEST)
    query_cos = jnp.dot(onehot, cos[...], **exact)
    query_sin = jnp.dot(onehot, sin[...], **exact)
    lane = lax.broadcasted_iota(jnp.int32, (1, LANES), 1)
    first = lane % head_size < head_size // 2

    def rotate(inputs, cosine, sine):
        turned = jnp.where(
            first,
            pltpu.roll(inputs, LANES - head_size // 2, 1),
            pltpu.roll(inputs, head_size // 2, 1),
        )
        return inputs * cosine + turned * sine

    transposed = (((1,), (1,)), ((), ()))
    low = lane < head_size
    span = seq_span // 2 if seq_span % 32 == 0 else seq_span
    head_rows = 3 * head_size

    def attend(relation, chunk):
        weights = wbuf.at[relation, chunk]
        pairs = [
            weights[head * head_rows + head_size : (head + 1) * head_rows, :]
            for head in range(heads_in_chunk)
        ]
        pair_weights = pairs[0] if heads_in_chunk == 1 else jnp.concatenate(pairs, axis=0)

        def project(step, carry):
            rows = pl.ds(pl.multiple_of(step * span, 16), span)
            made = lax.dot_general(
                normed[rows, :], pair_weights, transposed, preferred_element_type=f32
            )
            for head in range(heads_in_chunk):
                block = made[:, head * LANES : (head + 1) * LANES]
                block = jnp.where(low, rotate(block, cos[rows, :], sin[rows, :]), block)
                pbuf[rows, head * LANES : (head + 1) * LANES] = block.astype(bf16)
            return carry

        lax.fori_loop(0, seq_span // span, project, 0)
        if heads_in_chunk == 1:
            query_weights = weights[: 2 * head_size, :]
        else:
            query_weights = jnp.concatenate(
                [weights[:head_size, :], weights[head_rows : head_rows + head_size, :]], axis=0
            )
        made = lax.dot_general(masked_rows, query_weights, transposed, preferred_element_type=f32)
        turned = rotate(made * head_size ** (-0.5), query_cos, query_sin)
        vectors = []
        for head in range(heads_in_chunk):
            query = turned if head == 0 else pltpu.roll(turned, head_size, 1)
            query = jnp.where(low, query, 0.0).astype(bf16)
            block = pbuf[:, head * LANES : (head + 1) * LANES]
            logits = lax.dot_general(query, block, transposed, preferred_element_type=f32)
            logits = jnp.where(alive, logits, -1e30)
            weight = jnp.exp(logits - jnp.max(logits, axis=-1, keepdims=True))
            probs = (weight / jnp.sum(weight, axis=-1, keepdims=True)).astype(bf16)
            vectors.append(jnp.dot(probs, block, preferred_element_type=f32))
        total = pltpu.roll(vectors[0], head_size, 1)
        if heads_in_chunk > 1:
            total = jnp.where(low, total, vectors[1])
        context[relation, chunk] = total[:, :chunk_heads].astype(bf16)

    def mix(relation):
        for chunk in range(chunks):
            rows = slice(chunk * chunk_heads, (chunk + 1) * chunk_heads)
            mixed[...] += jnp.dot(
                context[relation, chunk], obuf[relation, rows, :], preferred_element_type=f32
            )

    def fetch(*pairs):
        for pair in pairs:
            arrived(*pair)
            share(*pair)

    def attend_shared(relation, chunk):
        was_shared(relation, part(chunk, 0))
        was_shared(relation, part(chunk, 1))
        attend(relation, chunk)

    attend(0, 0)
    if routed:
        first_piece, second_piece = 2 * chunks, 2 * chunks + 1
        arrived(1, part(1, 0))
        relay(2, 1, part(1, 0))
        exchange(1, 1)
        share(1, part(1, 0))
        arrived(2, part(0, 0))
        relay(1, 2, part(0, 0))
        exchange(2, 0)
        share(2, part(0, 0))
        direct(1, part(0, 1))
        direct(2, part(1, 1))
        direct(1, first_piece)
        direct(2, second_piece)
        direct(1, second_piece)
        direct(2, first_piece)
    for chunk in range(1, chunks):
        attend(0, chunk)
    mix(0)
    if routed:
        fetch((1, part(0, 0)), (2, part(1, 0)), (1, part(1, 1)))
        arrived(3, part(0, 0))
        exchange(3, 0)
        share(3, part(0, 0))
        arrived(3, part(1, 0))
        exchange(3, 1)
        share(3, part(1, 0))
        fetch((2, part(0, 1)))
        attend_shared(1, 1)
        attend_shared(2, 0)
        fetch((1, part(0, 1)), (2, part(1, 1)), (3, part(0, 1)))
        attend_shared(1, 0)
        arrived(1, first_piece)
        relay(2, 1, first_piece)
        share(1, first_piece)
        arrived(2, second_piece)
        relay(1, 2, second_piece)
        share(2, second_piece)
        attend_shared(2, 1)
        fetch((3, part(1, 1)))
        attend_shared(3, 0)
        fetch((1, second_piece), (2, first_piece))
        attend_shared(3, 1)
        for relation in (1, 2):
            was_shared(relation, first_piece)
            was_shared(relation, second_piece)
            mix(relation)
        fetch((3, first_piece), (3, second_piece))
        was_shared(3, first_piece)
        was_shared(3, second_piece)
        mix(3)
    else:
        for relation in range(1, n_mp):
            fetch(*[(relation, item) for item in range(items)])
        for relation in range(1, n_mp):
            for item in range(items):
                was_shared(relation, item)
            for chunk in range(chunks):
                attend(relation, chunk)
            mix(relation)

    normed_final = (layer_norm(mixed[...]) * final_gain_ref[...].reshape(1, feature)).astype(bf16)
    dense_copy.wait()
    dense_out = jnp.dot(normed_final, dense[...], preferred_element_type=f32)
    headed = layer_norm(0.5 * dense_out * (1.0 + lax.erf(dense_out * 0.5**0.5))).astype(bf16)
    logits = lax.dot_general(headed, decoder_ref[...], transposed, preferred_element_type=f32) + bias_ref[...]
    largest = jnp.max(logits, axis=-1, keepdims=True)
    scale = jnp.log(jnp.sum(jnp.exp(logits - largest), axis=-1, keepdims=True)) + largest
    vocabulary = lax.broadcasted_iota(jnp.int32, logits.shape, 1).astype(f32)
    picked = jnp.sum(jnp.where(vocabulary == targets, logits - scale, 0.0), axis=1, keepdims=True)
    row = jnp.sum(jnp.where(eye, picked, 0.0), axis=0, keepdims=True)
    padded = jnp.pad(row, ((0, 0), (0, LANES - masks)))
    scores[me] = jnp.broadcast_to(padded, scores.shape[1:])

    def score_copy(step):
        other = (me + step) % devices
        return pltpu.make_async_remote_copy(
            src_ref=scores.at[me, pl.ds(0, 1), :],
            dst_ref=scores.at[me, pl.ds(0, 1), :],
            send_sem=score_send_sem.at[step],
            recv_sem=score_sem.at[me],
            device_id=(other // n_mp, other % n_mp),
            device_id_type=MESH,
        )

    def send_scores(step, carry):
        score_copy(step).start()
        return carry

    lax.fori_loop(1, devices, send_scores, 0)
    for copy in sent:
        copy.wait_send()

    def wait_scores(step, carry):
        source = (me + step) % devices
        landing = scores.at[source, pl.ds(0, 1), :]
        pltpu.make_async_copy(landing, landing, score_sem.at[source]).wait()
        return carry

    lax.fori_loop(1, devices, wait_scores, 0)

    def wait_sends(step, carry):
        score_copy(step).wait_send()
        return carry

    lax.fori_loop(1, devices, wait_sends, 0)
    group = out_ref.shape[0]
    wanted = dp * group + lax.broadcasted_iota(jnp.int32, (group, owner_ref.shape[1]), 0)
    select = jnp.where(owner_ref[...] == wanted, 1.0, 0.0)
    out_ref[...] = jnp.dot(select, scores[:, 0, :], **exact)


def on_device(
    shape,
    hidden_states,
    ln_attn_gain,
    w_qkv,
    output_weight,
    ln_final_gain,
    dense_weight,
    decoder_weight,
    decoder_bias,
    seq_tokens,
    seq_lengths,
    copy_sequence,
    mask_code,
    copy_owner,
):
    n_dp, n_mp = shape
    devices = n_dp * n_mp
    lane_copies, seq_span, feature = hidden_states.shape
    head_size, heads, _ = output_weight.shape
    copies, masks = mask_code.shape
    assert lane_copies == 1 and copies == devices and n_dp % 2 == 0
    assert 2 * head_size == LANES and masks <= LANES
    in_chunk = 2 if heads % 2 == 0 else 1
    chunks = heads // in_chunk
    width = in_chunk * 3 * head_size
    weight = jnp.transpose(w_qkv.reshape(feature, chunks, width), (1, 2, 0))
    out_weight = jnp.swapaxes(output_weight, 0, 1).reshape(heads * head_size, feature)
    cosine, sine = rotary_tables(seq_span, head_size)
    group = copies // n_dp
    items = 2 * chunks + 2
    dma = pltpu.SemaphoreType.DMA
    vmem = pl.BlockSpec(memory_space=pltpu.VMEM)
    smem = pl.BlockSpec(memory_space=pltpu.SMEM)
    anywhere = pl.BlockSpec(memory_space=pl.ANY)
    rows = pl.pallas_call(
        functools.partial(kernel, (n_dp, n_mp, head_size, in_chunk, chunks)),
        name="score_copies",
        out_shape=jax.ShapeDtypeStruct((group, LANES), f32),
        in_specs=[smem] * 2 + [vmem] * 7 + [anywhere] * 6,
        out_specs=vmem,
        scratch_shapes=[
            pltpu.VMEM((seq_span, feature), bf16),
            pltpu.VMEM((seq_span, feature), bf16),
            pltpu.VMEM((n_mp, chunks, width, feature), bf16),
            pltpu.VMEM((n_mp, heads * head_size, feature), bf16),
            pltpu.VMEM((feature, feature), bf16),
            pltpu.VMEM((seq_span, LANES), f32),
            pltpu.VMEM((seq_span, LANES), f32),
            pltpu.VMEM((seq_span, in_chunk * LANES), bf16),
            pltpu.VMEM((n_mp, chunks, masks, in_chunk * head_size), bf16),
            pltpu.VMEM((masks, feature), f32),
            pltpu.VMEM((devices, 8, LANES), f32),
            dma((6,)),
            dma((n_mp, items)),
            dma((items,)),
            dma((n_mp, chunks)),
            dma((n_mp, items)),
            dma((n_mp, items)),
            dma((n_mp, items)),
            dma((devices,)),
            dma((devices,)),
        ],
        compiler_params=pltpu.CompilerParams(collective_id=0, has_side_effects=True),
    )(
        copy_sequence,
        seq_lengths,
        mask_code,
        seq_tokens,
        copy_owner.reshape(1, -1),
        ln_attn_gain,
        ln_final_gain,
        decoder_weight.T,
        decoder_bias.reshape(1, -1),
        hidden_states.reshape(seq_span, feature),
        weight,
        out_weight,
        dense_weight,
        jnp.asarray(cosine),
        jnp.asarray(sine),
    )
    own = masks // n_mp
    return lax.dynamic_slice_in_dim(rows, lax.axis_index("mp") * own, own, 1)


def solution(mesh):
    placed = (
        P(("dp", "mp"), None, None),
        P(),
        P(None, "mp", None),
        P(None, "mp", None),
        P(),
        P(),
        P(),
        P(),
        P(),
        P(),
        P(),
        P(),
        P(),
    )
    shape = (mesh.shape["dp"], mesh.shape["mp"])
    return jax.shard_map(
        functools.partial(on_device, shape),
        mesh=mesh,
        in_specs=placed,
        out_specs=P("dp", "mp"),
        check_vma=False,
    )
```

```python
import functools

import jax
import jax.numpy as jnp
import numpy as np
from jax import lax
from jax.experimental import pallas as pl
from jax.experimental.pallas import tpu as pltpu
from jax.sharding import PartitionSpec as P

epsilon = 1e-05
MESH = pl.DeviceIdType.MESH
f32 = jnp.float32
bf16 = jnp.bfloat16
LANES = 128


def layer_norm(inputs):
    average = jnp.mean(inputs, axis=-1, keepdims=True)
    centred = inputs - average
    variance = jnp.mean(centred * centred, axis=-1, keepdims=True)
    return centred * lax.rsqrt(variance + epsilon)


def rotary_tables(seq_span, head_size):
    half = head_size // 2
    frequency = (1.0 / 10000.0 ** (np.arange(half, dtype=np.float32) * (2.0 / head_size))).astype(
        np.float32
    )
    angles = np.arange(seq_span, dtype=np.float32)[:, None] * frequency[None, :]
    cosine, sine = np.cos(angles), np.sin(angles)
    times = LANES // head_size
    return (
        np.tile(np.concatenate([cosine, cosine], axis=1), (1, times)).astype(np.float32),
        np.tile(np.concatenate([-sine, sine], axis=1), (1, times)).astype(np.float32),
    )


def flip(index, mask):
    bit = 1
    out = index
    while bit <= mask:
        if mask & bit:
            out = out + bit * (1 - 2 * ((index // bit) % 2))
        bit *= 2
    return out


def kernel(
    sizes,
    sequence_ref,
    lengths_ref,
    codes_ref,
    tokens_ref,
    owner_ref,
    gain_ref,
    final_gain_ref,
    decoder_ref,
    bias_ref,
    hidden_hbm,
    weight_hbm,
    out_weight_hbm,
    dense_hbm,
    cos_hbm,
    sin_hbm,
    out_ref,
    hidden,
    normed,
    wbuf,
    obuf,
    dense,
    cos,
    sin,
    pbuf,
    context,
    mixed,
    scores,
    local_sem,
    direct_sem,
    relay_sem,
    exchange_sem,
    share_sem,
    arrive_sem,
    shared_sem,
    score_send_sem,
    score_sem,
):
    n_dp, n_mp, head_size, heads_in_chunk, chunks = sizes
    devices = n_dp * n_mp
    dp = lax.axis_index("dp")
    mp = lax.axis_index("mp")
    core = dp % 2
    partner = dp + 1 - 2 * core
    me = dp * n_mp + mp
    seq_span, feature = hidden.shape
    masks = codes_ref.shape[1]
    chunk_heads = heads_in_chunk * head_size
    out_rows = obuf.shape[1]
    piece_rows = out_rows // 4

    def local(index, source, target):
        copy = pltpu.make_async_copy(source, target, local_sem.at[index])
        copy.start()
        return copy

    weight_copy = local(1, weight_hbm, wbuf.at[0])
    hidden_copy = local(0, hidden_hbm, hidden)

    barrier = pltpu.get_barrier_semaphore()

    def greet(step, carry):
        other = (me + step) % devices
        pl.semaphore_signal(
            barrier, inc=1, device_id=(other // n_mp, other % n_mp), device_id_type=MESH
        )
        return carry

    lax.fori_loop(1, devices, greet, 0)

    parity = (dp // 2) % 2
    above = dp + 2 - 4 * parity
    part_rows = wbuf.shape[2] // 4

    def part(chunk, odd):
        return 2 * chunk + odd

    def place(relation, item, half):
        if item < 2 * chunks:
            chunk, odd = divmod(item, 2)
            which = 1 - parity if odd else parity
            start = (2 * half + which) * part_rows
            return wbuf.at[relation, chunk, pl.ds(pl.multiple_of(start, 16), part_rows), :]
        start = (2 * half + item - 2 * chunks) * piece_rows
        return obuf.at[relation, pl.ds(pl.multiple_of(start, 16), piece_rows), :]

    def view(relation, item):
        return place(relation, item, core)

    def partner_view(relation, item):
        return place(relation, item, 1 - core)

    sent = []

    def to_group(target, source_relation, relation, item, semaphore):
        copy = pltpu.make_async_remote_copy(
            src_ref=view(source_relation, item),
            dst_ref=view(relation, item),
            send_sem=semaphore,
            recv_sem=arrive_sem.at[relation, item],
            device_id=(dp, flip(mp, target)),
            device_id_type=MESH,
        )
        copy.start()
        sent.append(copy)

    def direct(target, item):
        to_group(target, 0, target, item, direct_sem.at[target, item])

    def relay(target, source_relation, item):
        to_group(target, source_relation, source_relation ^ target, item, relay_sem.at[item])

    def exchange(relation, chunk):
        copy = pltpu.make_async_remote_copy(
            src_ref=view(relation, part(chunk, 0)),
            dst_ref=view(relation, part(chunk, 0)),
            send_sem=exchange_sem.at[relation, chunk],
            recv_sem=arrive_sem.at[relation, part(chunk, 1)],
            device_id=(above, mp),
            device_id_type=MESH,
        )
        copy.start()
        sent.append(copy)

    def arrived(relation, item):
        landing = view(relation, item)
        pltpu.make_async_copy(landing, landing, arrive_sem.at[relation, item]).wait()

    def share(relation, item):
        copy = pltpu.make_async_remote_copy(
            src_ref=view(relation, item),
            dst_ref=view(relation, item),
            send_sem=share_sem.at[relation, item],
            recv_sem=shared_sem.at[relation, item],
            device_id=(partner, mp),
            device_id_type=MESH,
        )
        copy.start()
        sent.append(copy)

    def was_shared(relation, item):
        landing = partner_view(relation, item)
        pltpu.make_async_copy(landing, landing, shared_sem.at[relation, item]).wait()

    sequence = sequence_ref[me]
    length = lengths_ref[sequence].astype(f32)
    codes = codes_ref[pl.ds(me, 1), :].astype(f32)
    quotient = jnp.floor(codes / length)
    row_positions = codes - quotient * length
    row_positions = jnp.where(row_positions < 0.0, row_positions + length, row_positions)
    row_positions = jnp.where(row_positions >= length, row_positions - length, row_positions)
    eye = lax.broadcasted_iota(jnp.int32, (masks, masks), 0) == lax.broadcasted_iota(
        jnp.int32, (masks, masks), 1
    )
    positions = jnp.sum(jnp.where(eye, row_positions, 0.0), axis=1, keepdims=True)
    places = lax.broadcasted_iota(jnp.int32, (masks, seq_span), 1).astype(f32)
    chosen = places == positions
    onehot = jnp.where(chosen, 1.0, 0.0)
    onehot_bf = onehot.astype(bf16)
    tokens = tokens_ref[pl.ds(sequence, 1), :].astype(f32)
    targets = jnp.sum(jnp.where(chosen, tokens, 0.0), axis=1, keepdims=True)
    alive = lax.broadcasted_iota(jnp.int32, (1, seq_span), 1).astype(f32) < length

    weight_copy.wait()
    pl.semaphore_wait(barrier, devices - 1)
    items = 2 * chunks + 2
    routed = n_mp == 4 and chunks == 2 and n_dp % 4 == 0
    if routed:
        direct(1, part(1, 0))
        direct(2, part(0, 0))
        direct(1, part(0, 0))
        direct(2, part(1, 0))
    cos_copy = local(3, cos_hbm, cos)
    sin_copy = local(4, sin_hbm, sin)
    out_weight_copy = local(2, out_weight_hbm, obuf.at[0])
    dense_copy = local(5, dense_hbm, dense)
    if not routed:
        out_weight_copy.wait()
        for item in range(items):
            for target in range(1, n_mp):
                direct(target, item)

    hidden_copy.wait()
    tile = 128 if seq_span % 128 == 0 else 8

    def norm_rows(step, carry):
        rows = pl.ds(pl.multiple_of(step * tile, tile), tile)
        normed[rows, :] = (layer_norm(hidden[rows, :].astype(f32)) * gain_ref[...].reshape(1, feature)).astype(bf16)
        return carry

    lax.fori_loop(0, seq_span // tile, norm_rows, 0)
    masked_rows = jnp.dot(onehot_bf, normed[...], preferred_element_type=f32).astype(bf16)
    own_rows = jnp.dot(onehot_bf, hidden[...], preferred_element_type=f32)
    mixed[...] = own_rows
    cos_copy.wait()
    sin_copy.wait()
    exact = dict(preferred_element_type=f32, precision=lax.Precision.HIGHEST)
    query_cos = jnp.dot(onehot, cos[...], **exact)
    query_sin = jnp.dot(onehot, sin[...], **exact)
    lane = lax.broadcasted_iota(jnp.int32, (1, LANES), 1)
    first = lane % head_size < head_size // 2

    def rotate(inputs, cosine, sine):
        turned = jnp.where(
            first,
            pltpu.roll(inputs, LANES - head_size // 2, 1),
            pltpu.roll(inputs, head_size // 2, 1),
        )
        return inputs * cosine + turned * sine

    transposed = (((1,), (1,)), ((), ()))
    low = lane < head_size
    span = seq_span // 2 if seq_span % 32 == 0 else seq_span
    head_rows = 3 * head_size

    def attend(relation, chunk):
        weights = wbuf.at[relation, chunk]
        pairs = [
            weights[head * head_rows + head_size : (head + 1) * head_rows, :]
            for head in range(heads_in_chunk)
        ]
        pair_weights = pairs[0] if heads_in_chunk == 1 else jnp.concatenate(pairs, axis=0)

        def project(step, carry):
            rows = pl.ds(pl.multiple_of(step * span, 16), span)
            made = lax.dot_general(
                normed[rows, :], pair_weights, transposed, preferred_element_type=f32
            )
            for head in range(heads_in_chunk):
                block = made[:, head * LANES : (head + 1) * LANES]
                block = jnp.where(low, rotate(block, cos[rows, :], sin[rows, :]), block)
                pbuf[rows, head * LANES : (head + 1) * LANES] = block.astype(bf16)
            return carry

        lax.fori_loop(0, seq_span // span, project, 0)
        if heads_in_chunk == 1:
            query_weights = weights[: 2 * head_size, :]
        else:
            query_weights = jnp.concatenate(
                [weights[:head_size, :], weights[head_rows : head_rows + head_size, :]], axis=0
            )
        made = lax.dot_general(masked_rows, query_weights, transposed, preferred_element_type=f32)
        turned = rotate(made * head_size ** (-0.5), query_cos, query_sin)
        vectors = []
        for head in range(heads_in_chunk):
            query = turned if head == 0 else pltpu.roll(turned, head_size, 1)
            query = jnp.where(low, query, 0.0).astype(bf16)
            block = pbuf[:, head * LANES : (head + 1) * LANES]
            logits = lax.dot_general(query, block, transposed, preferred_element_type=f32)
            logits = jnp.where(alive, logits, -1e30)
            weight = jnp.exp(logits - jnp.max(logits, axis=-1, keepdims=True))
            probs = (weight / jnp.sum(weight, axis=-1, keepdims=True)).astype(bf16)
            vectors.append(jnp.dot(probs, block, preferred_element_type=f32))
        total = pltpu.roll(vectors[0], head_size, 1)
        if heads_in_chunk > 1:
            total = jnp.where(low, total, vectors[1])
        context[relation, chunk] = total[:, :chunk_heads].astype(bf16)

    def mix(relation):
        for chunk in range(chunks):
            rows = slice(chunk * chunk_heads, (chunk + 1) * chunk_heads)
            mixed[...] += jnp.dot(
                context[relation, chunk], obuf[relation, rows, :], preferred_element_type=f32
            )

    def fetch(*pairs):
        for pair in pairs:
            arrived(*pair)
            share(*pair)

    def attend_shared(relation, chunk):
        was_shared(relation, part(chunk, 0))
        was_shared(relation, part(chunk, 1))
        attend(relation, chunk)

    attend(0, 0)
    if routed:
        first_piece, second_piece = 2 * chunks, 2 * chunks + 1
        arrived(1, part(1, 0))
        relay(2, 1, part(1, 0))
        exchange(1, 1)
        share(1, part(1, 0))
        arrived(2, part(0, 0))
        relay(1, 2, part(0, 0))
        exchange(2, 0)
        share(2, part(0, 0))
        direct(1, part(0, 1))
        direct(2, part(1, 1))
        out_weight_copy.wait()
        direct(1, first_piece)
        direct(2, second_piece)
        direct(1, second_piece)
        direct(2, first_piece)
    for chunk in range(1, chunks):
        attend(0, chunk)
    mix(0)
    if routed:
        fetch((1, part(0, 0)), (2, part(1, 0)), (1, part(1, 1)))
        arrived(3, part(0, 0))
        exchange(3, 0)
        share(3, part(0, 0))
        arrived(3, part(1, 0))
        exchange(3, 1)
        share(3, part(1, 0))
        fetch((2, part(0, 1)))
        attend_shared(1, 1)
        attend_shared(2, 0)
        fetch((1, part(0, 1)), (2, part(1, 1)), (3, part(0, 1)))
        attend_shared(1, 0)
        arrived(1, first_piece)
        relay(2, 1, first_piece)
        share(1, first_piece)
        arrived(2, second_piece)
        relay(1, 2, second_piece)
        share(2, second_piece)
        attend_shared(2, 1)
        fetch((3, part(1, 1)))
        attend_shared(3, 0)
        fetch((1, second_piece), (2, first_piece))
        attend_shared(3, 1)
        for relation in (1, 2):
            was_shared(relation, first_piece)
            was_shared(relation, second_piece)
            mix(relation)
        fetch((3, first_piece), (3, second_piece))
        was_shared(3, first_piece)
        was_shared(3, second_piece)
        mix(3)
    else:
        for relation in range(1, n_mp):
            fetch(*[(relation, item) for item in range(items)])
        for relation in range(1, n_mp):
            for item in range(items):
                was_shared(relation, item)
            for chunk in range(chunks):
                attend(relation, chunk)
            mix(relation)

    normed_final = (layer_norm(mixed[...]) * final_gain_ref[...].reshape(1, feature)).astype(bf16)
    dense_copy.wait()
    dense_out = jnp.dot(normed_final, dense[...], preferred_element_type=f32)
    headed = layer_norm(0.5 * dense_out * (1.0 + lax.erf(dense_out * 0.5**0.5))).astype(bf16)
    logits = lax.dot_general(headed, decoder_ref[...], transposed, preferred_element_type=f32) + bias_ref[...]
    largest = jnp.max(logits, axis=-1, keepdims=True)
    scale = jnp.log(jnp.sum(jnp.exp(logits - largest), axis=-1, keepdims=True)) + largest
    vocabulary = lax.broadcasted_iota(jnp.int32, logits.shape, 1).astype(f32)
    picked = jnp.sum(jnp.where(vocabulary == targets, logits - scale, 0.0), axis=1, keepdims=True)
    row = jnp.sum(jnp.where(eye, picked, 0.0), axis=0, keepdims=True)
    padded = jnp.pad(row, ((0, 0), (0, LANES - masks)))
    scores[me] = jnp.broadcast_to(padded, scores.shape[1:])

    def score_copy(step):
        other = (me + step) % devices
        return pltpu.make_async_remote_copy(
            src_ref=scores.at[me, pl.ds(0, 1), :],
            dst_ref=scores.at[me, pl.ds(0, 1), :],
            send_sem=score_send_sem.at[step],
            recv_sem=score_sem.at[me],
            device_id=(other // n_mp, other % n_mp),
            device_id_type=MESH,
        )

    def send_scores(step, carry):
        score_copy(step).start()
        return carry

    lax.fori_loop(1, devices, send_scores, 0)
    for copy in sent:
        copy.wait_send()

    def wait_scores(step, carry):
        source = (me + step) % devices
        landing = scores.at[source, pl.ds(0, 1), :]
        pltpu.make_async_copy(landing, landing, score_sem.at[source]).wait()
        return carry

    lax.fori_loop(1, devices, wait_scores, 0)

    def wait_sends(step, carry):
        score_copy(step).wait_send()
        return carry

    lax.fori_loop(1, devices, wait_sends, 0)
    group = out_ref.shape[0]
    wanted = dp * group + lax.broadcasted_iota(jnp.int32, (group, owner_ref.shape[1]), 0)
    select = jnp.where(owner_ref[...] == wanted, 1.0, 0.0)
    out_ref[...] = jnp.dot(select, scores[:, 0, :], **exact)


def on_device(
    shape,
    hidden_states,
    ln_attn_gain,
    w_qkv,
    output_weight,
    ln_final_gain,
    dense_weight,
    decoder_weight,
    decoder_bias,
    seq_tokens,
    seq_lengths,
    copy_sequence,
    mask_code,
    copy_owner,
):
    n_dp, n_mp = shape
    devices = n_dp * n_mp
    lane_copies, seq_span, feature = hidden_states.shape
    head_size, heads, _ = output_weight.shape
    copies, masks = mask_code.shape
    assert lane_copies == 1 and copies == devices and n_dp % 2 == 0
    assert 2 * head_size == LANES and masks <= LANES
    in_chunk = 2 if heads % 2 == 0 else 1
    chunks = heads // in_chunk
    width = in_chunk * 3 * head_size
    weight = jnp.transpose(w_qkv.reshape(feature, chunks, width), (1, 2, 0))
    out_weight = jnp.swapaxes(output_weight, 0, 1).reshape(heads * head_size, feature)
    cosine, sine = rotary_tables(seq_span, head_size)
    group = copies // n_dp
    items = 2 * chunks + 2
    dma = pltpu.SemaphoreType.DMA
    vmem = pl.BlockSpec(memory_space=pltpu.VMEM)
    smem = pl.BlockSpec(memory_space=pltpu.SMEM)
    anywhere = pl.BlockSpec(memory_space=pl.ANY)
    rows = pl.pallas_call(
        functools.partial(kernel, (n_dp, n_mp, head_size, in_chunk, chunks)),
        name="score_copies",
        out_shape=jax.ShapeDtypeStruct((group, LANES), f32),
        in_specs=[smem] * 2 + [vmem] * 7 + [anywhere] * 6,
        out_specs=vmem,
        scratch_shapes=[
            pltpu.VMEM((seq_span, feature), bf16),
            pltpu.VMEM((seq_span, feature), bf16),
            pltpu.VMEM((n_mp, chunks, width, feature), bf16),
            pltpu.VMEM((n_mp, heads * head_size, feature), bf16),
            pltpu.VMEM((feature, feature), bf16),
            pltpu.VMEM((seq_span, LANES), f32),
            pltpu.VMEM((seq_span, LANES), f32),
            pltpu.VMEM((seq_span, in_chunk * LANES), bf16),
            pltpu.VMEM((n_mp, chunks, masks, in_chunk * head_size), bf16),
            pltpu.VMEM((masks, feature), f32),
            pltpu.VMEM((devices, 8, LANES), f32),
            dma((6,)),
            dma((n_mp, items)),
            dma((items,)),
            dma((n_mp, chunks)),
            dma((n_mp, items)),
            dma((n_mp, items)),
            dma((n_mp, items)),
            dma((devices,)),
            dma((devices,)),
        ],
        compiler_params=pltpu.CompilerParams(collective_id=0, has_side_effects=True),
    )(
        copy_sequence,
        seq_lengths,
        mask_code,
        seq_tokens,
        copy_owner.reshape(1, -1),
        ln_attn_gain,
        ln_final_gain,
        decoder_weight.T,
        decoder_bias.reshape(1, -1),
        hidden_states.reshape(seq_span, feature),
        weight,
        out_weight,
        dense_weight,
        jnp.asarray(cosine),
        jnp.asarray(sine),
    )
    own = masks // n_mp
    return lax.dynamic_slice_in_dim(rows, lax.axis_index("mp") * own, own, 1)


def solution(mesh):
    placed = (
        P(("dp", "mp"), None, None),
        P(),
        P(None, "mp", None),
        P(None, "mp", None),
        P(),
        P(),
        P(),
        P(),
        P(),
        P(),
        P(),
        P(),
        P(),
    )
    shape = (mesh.shape["dp"], mesh.shape["mp"])
    return jax.shard_map(
        functools.partial(on_device, shape),
        mesh=mesh,
        in_specs=placed,
        out_specs=P("dp", "mp"),
        check_vma=False,
    )
```
